32 devices in a mesh: dp: 16 (over z, x, core), tp: 2 (over y).
Axes of the slice: x: 2, y: 2, z: 4, core: 2. Of those that a mesh axis runs over, the one named last changes fastest.
Arguments:
- gate_pre: bfloat16 [12288, 7168], P('dp', 'tp'), may hold values from -6 to 6
- up_pre: bfloat16 [12288, 7168], P('dp', 'tp'), may hold values from -6 to 6
- target: bfloat16 [12288, 2048], P('dp', 'tp'), may hold values from -6 to 6
- norm_gain: float32 [2048], P('tp'), may hold values from 0.5 to 1.5
- weight: bfloat16 [16, 7168, 2048], P('dp', 'tp'), may hold values from -6 to 6
- round_index: int32 [1], replicated, may hold values from 0 to 9999
Outputs:
- normed: bfloat16 [12288, 2048], P('dp', 'tp')
- mixed: bfloat16 [16, 7168, 2048], P('dp', 'tp')
The draws below stay inside these ranges and needn't reach their ends.
All inputs are finite; a program needn't handle non-finite values.
Results may differ from the reference program's by a relative error of at most 0.001.
The reference program's roundings to bfloat16 on the way (of `hidden`, `grad_out` and `updated`) count: a program that leaves them out, or rounds other values in their place, can miss the bound.
Values may be sent and summed in bfloat16 or wider, within the bound.
A program may use at most 128 MiB of HBM per device.

```python
import math
import jax
import jax.numpy as jnp
from jax import lax

D = 2048
FF = 7168
TOK = 768
TOKENS = 12288
N_DP = 16


def block_scale(key, dims, pieces, smallest, high):
    factor_of, own = 1.0, jax.random.fold_in(key, 6)
    for dim, shards_of in pieces:
        steps = jnp.exp(jax.random.uniform(jax.random.fold_in(own, dim), (shards_of,), jnp.float32, smallest / len(pieces), high / len(pieces)))
        factor_of = factor_of * jnp.repeat(steps, dims[dim] // shards_of).reshape([-1 if axis == dim else 1 for axis in range(len(dims))])
    return factor_of


def centred(key, extent, scale, reach, split=(), kind=jnp.bfloat16):
    drawn = jax.random.normal(key, extent, jnp.float32) * scale
    if len(split) > 0:
        drawn = block_scale(key, extent, split, -0.22, 0.18) * drawn
    return jnp.clip(drawn, min=-reach, max=reach).astype(kind)


def setup_inputs(seed: int = 0) -> dict:
    arg_keys = jax.random.split(jax.random.key(seed), 7)
    gate_pre = centred(arg_keys[0], (TOKENS, FF), 1.0, 6.0, ((0, 16), (1, 2)))
    up_pre = centred(arg_keys[1], (TOKENS, FF), 1.0, 6.0, ((0, 16), (1, 2)))
    target = centred(arg_keys[2], (TOKENS, D), 1.0, 6.0, ((0, 16), (1, 2)))
    norm_gain = jnp.clip(1.0 + 0.1 * jax.random.normal(arg_keys[3], (D,), jnp.float32), 0.5, 1.5)
    weight = centred(arg_keys[4], (N_DP, FF, D), 1.0, 6.0, ((0, 16), (1, 2)))
    round_index = jax.random.randint(arg_keys[5], (1,), 0, 10000).astype(jnp.int32)
    return {"gate_pre": gate_pre, "up_pre": up_pre, "target": target, "norm_gain": norm_gain, "weight": weight, "round_index": round_index}


EPSILON = 1e-06

def step_rate(round_index):
    phase = (round_index[0] % 1000).astype(jnp.float32) * jnp.float32(2.0 * math.pi / 1000.0)
    return jnp.float32(0.25) * (jnp.float32(0.55) + jnp.float32(0.45) * jnp.cos(phase))

def replica_step(inputs, norm_gain, rate):
    gate_rows, up_rows, target_rows, weight_rows = inputs
    out_scale = FF ** (-0.5)
    hidden = (jax.nn.silu(gate_rows.astype(jnp.float32)) * up_rows.astype(jnp.float32)).astype(jnp.bfloat16)
    summed = jnp.dot(hidden, weight_rows, preferred_element_type=jnp.float32) * out_scale
    inv_rms = lax.rsqrt(lax.optimization_barrier(jnp.mean(summed * summed, axis=1, keepdims=True)) + EPSILON)
    normal = summed * inv_rms
    output = normal * norm_gain
    grad_norm = (output - target_rows.astype(jnp.float32)) * norm_gain
    inner = lax.optimization_barrier(jnp.mean(grad_norm * normal, axis=1, keepdims=True))
    grad_out = (inv_rms * (grad_norm - normal * inner)).astype(jnp.bfloat16)
    weight_grad = lax.dot_general(hidden, grad_out, (((0,), (0,)), ((), ())), preferred_element_type=jnp.float32) * out_scale
    updated = (weight_rows.astype(jnp.float32) - rate * weight_grad).astype(jnp.bfloat16)
    return (output.astype(jnp.bfloat16), updated)

def reference(gate_pre, up_pre, target, norm_gain, weight, round_index):
    gate_blocks = gate_pre.reshape(N_DP, TOK, FF)
    up_blocks = up_pre.reshape(N_DP, TOK, FF)
    target_blocks = target.reshape(N_DP, TOK, D)
    rate = step_rate(round_index)

    def one_replica(inputs):
        return replica_step(inputs, norm_gain, rate)
    normed, updated = lax.map(one_replica, (gate_blocks, up_blocks, target_blocks, weight))
    levels = N_DP.bit_length() - 1
    offset = jnp.left_shift(jnp.int32(1), (round_index[0] % levels).astype(jnp.int32))
    source = ((jnp.arange(N_DP, dtype=jnp.int32) - offset) % N_DP).astype(jnp.int32)
    peer_rows = updated[source]
    mixed = (0.5 * (updated.astype(jnp.float32) + peer_rows.astype(jnp.float32))).astype(jnp.bfloat16)
    return (normed.reshape(N_DP * TOK, D), mixed)
```

```python
import math

import jax
import jax.numpy as jnp
from jax import lax
from jax.sharding import PartitionSpec as P

EPSILON = 1e-06


TOKEN_CHUNKS = 2
ROW_CHUNKS = 4


def shifted(array, axis, by):
    count = lax.axis_size(axis)
    return lax.ppermute(array, axis, [(i, (i + by) % count) for i in range(count)])


def step_rate(round_index):
    phase = (round_index[0] % 1000).astype(jnp.float32) * jnp.float32(2.0 * math.pi / 1000.0)
    return jnp.float32(0.25) * (jnp.float32(0.55) + jnp.float32(0.45) * jnp.cos(phase))


def total_over_tp(values):
    total = values
    for k in range(1, lax.axis_size("tp")):
        total = total + shifted(values, "tp", k)
    return total


def shards(gate_pre, up_pre, target, norm_gain, weight, round_index):
    rate = step_rate(round_index)
    levels = lax.axis_size("dp").bit_length() - 1
    level = round_index[0] % levels
    tp = lax.axis_size("tp")
    me = lax.axis_index("tp")
    weight_rows = weight[0]
    rows, width = weight_rows.shape
    tokens = gate_pre.shape[0]
    part = width // tp
    scale = (rows * tp) ** (-0.5)

    def columns(k):
        return lax.rem(me + k + tp, tp) * part

    def weight_block(k):
        return lax.dynamic_slice(weight_rows, (0, columns(k)), (rows, part))

    hidden = (jax.nn.silu(gate_pre.astype(jnp.float32)) * up_pre.astype(jnp.float32)).astype(
        jnp.bfloat16
    )
    pieces = TOKEN_CHUNKS if tokens % (TOKEN_CHUNKS * 128) == 0 else 1
    piece = tokens // pieces

    def partial(first, count, k):
        return jnp.dot(
            hidden[first : first + count], weight_block(k), preferred_element_type=jnp.float32
        ) * scale

    arrived = [
        [shifted(partial(i * piece, piece, k), "tp", k) for i in range(pieces)]
        for k in range(1, tp)
    ]
    share = partial(0, tokens, 0)
    for parts in arrived:
        share = share + jnp.concatenate(parts, axis=0)

    square_sum = total_over_tp(jnp.sum(share * share, axis=1))[:, None]
    inv_rms = lax.rsqrt(square_sum / width + EPSILON)
    normal = share * inv_rms
    output = normal * norm_gain
    grad_norm = (output - target.astype(jnp.float32)) * norm_gain
    inner_sum = total_over_tp(jnp.sum(grad_norm * normal, axis=1))[:, None]
    grad_share = (inv_rms * (grad_norm - normal * (inner_sum / width))).astype(jnp.bfloat16)
    normed = output.astype(jnp.bfloat16)

    def updated(grad_cols, k):
        weight_grad = lax.dot_general(
            hidden, grad_cols, (((0,), (0,)), ((), ())), preferred_element_type=jnp.float32
        ) * scale
        return (weight_block(-k).astype(jnp.float32) - rate * weight_grad).astype(jnp.bfloat16)

    count = rows // ROW_CHUNKS

    def branch(bit):
        def run(own_first, grad_share):
            mixed = jnp.zeros((rows, width), jnp.bfloat16)
            for k in range(tp):
                own = updated(shifted(grad_share, "tp", k), k) if k else own_first
                for i in range(ROW_CHUNKS):
                    first = i * count
                    last = first + count if i < ROW_CHUNKS - 1 else rows
                    block = own[first:last]
                    peer = shifted(block, "dp", 1 << bit)
                    block = 0.5 * (block.astype(jnp.float32) + peer.astype(jnp.float32))
                    mixed = lax.dynamic_update_slice(
                        mixed, block.astype(jnp.bfloat16), (first, columns(-k))
                    )
            return mixed

        return run

    mixed = lax.switch(
        level, [branch(bit) for bit in range(levels)], updated(grad_share, 0), grad_share
    )
    return (normed, mixed[None])


def solution(mesh):
    return jax.shard_map(
        shards,
        mesh=mesh,
        in_specs=(P("dp", "tp"), P("dp", "tp"), P("dp", "tp"), P("tp"), P("dp", "tp", None), P()),
        out_specs=(P("dp", "tp"), P("dp", "tp", None)),
        check_vma=False,
    )
```
